8 devices in a mesh: dp: 1 (over z), tp: 8 (over x, y, core).
Axes of the slice: x: 2, y: 2, z: 1, core: 2. Of those that a mesh axis runs over, the one named last changes fastest.
Arguments:
- x: bfloat16 [64, 2048], P('dp')
- k_cache: bfloat16 [64, 4096, 32, 64], P('dp', None, 'tp')
- v_cache: bfloat16 [64, 4096, 32, 64], P('dp', None, 'tp')
- gain_a: bfloat16 [2048], replicated
- wq: bfloat16 [2048, 2048], P(None, 'tp')
- wo: bfloat16 [2048, 2048], P('tp')
- gain_m: bfloat16 [2048], replicated
- w_gate: bfloat16 [2048, 5120], P(None, 'tp')
- w_up: bfloat16 [2048, 5120], P(None, 'tp')
- w_down: bfloat16 [5120, 2048], P('tp')
Outputs:
- output: bfloat16 [64, 2048], P('dp')
All inputs are finite; a program needn't handle non-finite values.
Results may differ from the reference program's by a relative error of at most 0.017.
Values are sent between devices in bfloat16 or wider.
A program may use at most 2 GiB of HBM per device.

```python
import jax
import jax.numpy as jnp
from jax import lax

BATCH = 64
CACHE = 4096
D = 2048
HEADS = 32
KV_HEADS = 32
HEAD = 64
FF = 5120
THETA = 10000


def setup_inputs(seed: int = 0, part: int = 0) -> dict:
    kx, kc, kw, kn, kq, ko, km, kg, ku, kd = jax.random.split(jax.random.key(seed), 10)
    kx, kc, kw = (jax.random.fold_in(k, part) for k in (kx, kc, kw))

    def weights(key, rows, columns):
        return jax.random.normal(key, (rows, columns), jnp.float32) * rows**-0.5

    drawn = {
        "x": jax.random.normal(kx, (BATCH, D), jnp.float32),
        "k_cache": 2 * jax.random.normal(kc, (BATCH, CACHE, KV_HEADS, HEAD), jnp.float32),
        "v_cache": 4 * jax.random.normal(kw, (BATCH, CACHE, KV_HEADS, HEAD), jnp.float32),
        "gain_a": 1 + 0.1 * jax.random.normal(kn, (D,), jnp.float32),
        "wq": 2 * weights(kq, D, HEADS * HEAD),
        "wo": weights(ko, HEADS * HEAD, D),
        "gain_m": 1 + 0.1 * jax.random.normal(km, (D,), jnp.float32),
        "w_gate": weights(kg, D, FF),
        "w_up": weights(ku, D, FF),
        "w_down": 2 * weights(kd, FF, D),
    }
    return {k: v.astype(jnp.bfloat16) for k, v in drawn.items()}


def normed(x, gain):
    wide = x.astype(jnp.float32)
    scale = lax.rsqrt(jnp.mean(wide * wide, -1, keepdims=True) + 1e-6)
    return (wide * scale * gain.astype(jnp.float32)).astype(jnp.bfloat16)


def turned(t, place, theta):
    half = t.shape[-1] // 2
    angle = place.astype(jnp.float32)[:, None] * theta ** (-jnp.arange(half, dtype=jnp.float32) / half)
    cos, sin = jnp.cos(angle)[:, None], jnp.sin(angle)[:, None]
    a, b = t[..., :half].astype(jnp.float32), t[..., half:].astype(jnp.float32)
    return jnp.concatenate([a * cos - b * sin, b * cos + a * sin], -1).astype(jnp.bfloat16)


def matmul(a, w):
    return jnp.dot(a, w, preferred_element_type=jnp.float32).astype(jnp.bfloat16)


def einsum(form, a, b):
    return jnp.einsum(form, a.astype(jnp.float32), b.astype(jnp.float32))


def seen_by(a, wq, k_cache, v_cache, head, theta):
    batch, cache, kv_heads = k_cache.shape[:3]
    place = jnp.full((batch,), cache - 1)
    q = turned(matmul(a, wq).reshape(batch, -1, head), place, theta).reshape(batch, kv_heads, -1, head)
    scores = einsum("bgsd,bugd->bgsu", q, k_cache) * head**-0.5
    weights = jax.nn.softmax(scores, -1).astype(jnp.bfloat16)
    return einsum("bgsu,bugd->bgsd", weights, v_cache).astype(jnp.bfloat16).reshape(batch, -1)


def hidden_of(b, w_gate, w_up):
    gate = jnp.dot(b, w_gate, preferred_element_type=jnp.float32)
    up = jnp.dot(b, w_up, preferred_element_type=jnp.float32)
    return (jax.nn.silu(gate) * up).astype(jnp.bfloat16)


def reference(x, k_cache, v_cache, gain_a, wq, wo, gain_m, w_gate, w_up, w_down):
    seen = seen_by(normed(x, gain_a), wq, k_cache, v_cache, HEAD, THETA)
    h = (x.astype(jnp.float32) + jnp.dot(seen, wo, preferred_element_type=jnp.float32)).astype(jnp.bfloat16)
    hidden = hidden_of(normed(h, gain_m), w_gate, w_up)
    return (h.astype(jnp.float32) + jnp.dot(hidden, w_down, preferred_element_type=jnp.float32)).astype(jnp.bfloat16)
```

```python
import functools

import jax
import jax.numpy as jnp
import numpy as np
from jax import lax
from jax.experimental import pallas as pl
from jax.experimental.pallas import tpu as pltpu
from jax.sharding import PartitionSpec as P

HEAD = 64
THETA = 10000
EPS = 1e-6
SLOTS = 10
CHUNKS = (16, 16, 16, 8, 8)
MESH = pl.DeviceIdType.MESH
F32, BF16 = jnp.float32, jnp.bfloat16


def turn_table(place, heads):
    half = HEAD // 2
    angle = np.float32(place) * np.float32(THETA) ** (-np.arange(half, dtype=np.float32) / np.float32(half))
    angle = angle.astype(np.float32)
    cos, sin = np.cos(angle), np.sin(angle)
    return np.stack([np.tile(np.concatenate([cos, cos]), heads), np.tile(np.concatenate([-sin, sin]), heads)]).astype(np.float32)


def dot(a, b):
    return jnp.dot(a, b, preferred_element_type=F32)


def dot_t(a, b):
    return lax.dot_general(a, b, (((1,), (1,)), ((), ())), preferred_element_type=F32)


def normed(wide, gain):
    return (wide * lax.rsqrt(jnp.mean(wide * wide, -1, keepdims=True) + EPS) * gain).astype(BF16)


def kernel(n, k_hbm, v_hbm, x_hbm, ga_hbm, wq_hbm, wo_hbm, gm_hbm, wg_hbm, wu_hbm, wd_hbm, table_hbm, y_ref, *scratch):
    rows, width, cache = k_hbm.shape
    heads = width // HEAD
    hidden = wg_hbm.shape[1]
    (kbuf, vbuf, x_ref, ga, gm, table, wq, wo, wgu, wd, xf, hf, qf, seen, scores, ksem, vsem, wsem) = scratch[:18]
    chunks = len(CHUNKS)
    first, second = scratch[18 : 18 + chunks], scratch[18 + chunks : 18 + 2 * chunks]
    send_sem, recv_sem = scratch[18 + 2 * chunks :]
    me = lax.axis_index("tp")
    peers = [lax.rem(me + i, n) for i in range(1, n)]

    def kcopy(s):
        slot = lax.rem(s, SLOTS)
        return pltpu.make_async_copy(k_hbm.at[s], kbuf.at[slot], ksem.at[slot])

    def vcopy(s):
        slot = lax.rem(s, SLOTS)
        return pltpu.make_async_copy(v_hbm.at[s], vbuf.at[slot], vsem.at[slot])

    small = [
        pltpu.make_async_copy(src, dst, wsem.at[i])
        for i, (src, dst) in enumerate(
            [
                (x_hbm, x_ref),
                (ga_hbm, ga),
                (wq_hbm, wq),
                (table_hbm, table),
                (wo_hbm, wo),
                (gm_hbm, gm),
                (wg_hbm, wgu.at[:, :hidden]),
                (wu_hbm, wgu.at[:, hidden:]),
                (wd_hbm, wd),
            ]
        )
    ]
    for copy in small[:4]:
        copy.start()
    for s in range(SLOTS):
        kcopy(s).start()
        vcopy(s).start()
    for copy in small[4:]:
        copy.start()

    barrier = pltpu.get_barrier_semaphore()
    for peer in peers:
        pl.semaphore_signal(barrier, inc=1, device_id={"tp": peer}, device_id_type=MESH)

    for copy in small[:2]:
        copy.wait()
    xf[...] = x_ref[...].astype(F32)
    a = normed(xf[...], ga[...].astype(F32))
    for copy in small[2:4]:
        copy.wait()
    q = dot(a, wq[...]).astype(BF16).astype(F32)
    half = HEAD // 2
    lane = lax.broadcasted_iota(jnp.int32, q.shape, 1)
    other = jnp.where(lax.rem(lane, HEAD) < half, pltpu.roll(q, width - half, 1), pltpu.roll(q, half, 1))
    qf[...] = (q * table[0:1, :] + other * table[1:2, :]).astype(BF16).astype(F32)

    own = lax.broadcasted_iota(jnp.int32, (8, width), 1) // HEAD == lax.broadcasted_iota(jnp.int32, (8, width), 0)

    def score(s):
        query = jnp.where(own, jnp.broadcast_to(qf[pl.ds(s, 1), :], (8, width)), 0.0).astype(BF16)
        return dot(query, kbuf[lax.rem(s, SLOTS)])

    def attend(s, wide):
        scaled = wide * HEAD**-0.5
        e = jnp.exp(scaled - jnp.max(scaled, -1, keepdims=True))
        weights = (e * (1.0 / jnp.sum(e, -1, keepdims=True))).astype(BF16)
        out = dot_t(weights, vbuf[lax.rem(s, SLOTS)])
        seen[pl.ds(s, 1), :] = jnp.sum(jnp.where(own, out, 0.0), 0, keepdims=True)

    def step(s, _):
        kcopy(s + 1).wait()
        vcopy(s).wait()
        wide = scores[lax.rem(s, 2)]
        scores[lax.rem(s + 1, 2)] = score(s + 1)
        attend(s, wide)

        @pl.when(s + 1 + SLOTS < rows)
        def _():
            kcopy(s + 1 + SLOTS).start()

        @pl.when(s + SLOTS < rows)
        def _():
            vcopy(s + SLOTS).start()

        return 0

    def sends(half, c, buf):
        return [
            pltpu.make_async_remote_copy(
                src_ref=buf.at[me],
                dst_ref=buf.at[me],
                send_sem=send_sem.at[half, c, i],
                recv_sem=recv_sem.at[half, c, me],
                device_id={"tp": peer},
                device_id_type=MESH,
            )
            for i, peer in enumerate(peers)
        ]

    def receive(half, c, buf):
        for peer in peers:
            pltpu.make_async_remote_copy(
                src_ref=buf.at[peer],
                dst_ref=buf.at[peer],
                send_sem=send_sem.at[half, c, 0],
                recv_sem=recv_sem.at[half, c, peer],
                device_id={"tp": peer},
                device_id_type=MESH,
            ).wait_recv()
        total = buf[0].astype(F32)
        for i in range(1, n):
            total = total + buf[i].astype(F32)
        return total

    starts = [sum(CHUNKS[:c]) for c in range(chunks)]

    def project(c):
        part = slice(starts[c], starts[c] + CHUNKS[c])
        first[c][me] = dot(seen[part, :].astype(BF16), wo[...]).astype(BF16)
        for copy in sends(0, c, first[c]):
            copy.start()

    def feed(c):
        part = slice(starts[c], starts[c] + CHUNKS[c])
        h = (xf[part, :] + receive(0, c, first[c])).astype(BF16).astype(F32)
        hf[part, :] = h
        b = normed(h, gm[...].astype(F32))
        both = dot(b, wgu[...])
        gate, up = both[:, :hidden], both[:, hidden:]
        product = (gate * (1.0 / (1.0 + jnp.exp(-gate))) * up).astype(BF16)
        second[c][me] = dot(product, wd[...]).astype(BF16)
        for copy in sends(1, c, second[c]):
            copy.start()

    def finish(c):
        part = slice(starts[c], starts[c] + CHUNKS[c])
        y_ref[part, :] = (hf[part, :] + receive(1, c, second[c])).astype(BF16)

    kcopy(0).wait()
    scores[0] = score(0)
    for name in [0]:
        kcopy(SLOTS).start()
    for c in range(chunks):
        last = c == chunks - 1
        lax.fori_loop(starts[c], starts[c] + CHUNKS[c] - last, step, 0)
        if last:
            vcopy(rows - 1).wait()
            attend(rows - 1, scores[(rows - 1) % 2])
        if c == 0:
            for copy in small[4:]:
                copy.wait()
            pl.semaphore_wait(barrier, n - 1)
        project(c)
        if c >= 1:
            feed(c - 1)
        if c >= 2:
            finish(c - 2)
    feed(chunks - 1)
    finish(chunks - 2)
    finish(chunks - 1)
    for c in range(chunks):
        for half, buf in ((0, first[c]), (1, second[c])):
            for copy in sends(half, c, buf):
                copy.wait_send()


def solution(mesh):
    n = mesh.shape["tp"]

    def step(x, k_cache, v_cache, gain_a, wq, wo, gain_m, w_gate, w_up, w_down):
        rows, cache, heads, head = k_cache.shape
        d, width, hidden = x.shape[1], heads * head, w_gate.shape[1]
        flat = lambda t: t.transpose(0, 2, 3, 1).reshape(rows, width, cache)
        table = jnp.asarray(turn_table(cache - 1, heads))
        chunks = len(CHUNKS)
        scratch = [
            pltpu.VMEM((SLOTS, width, cache), BF16),
            pltpu.VMEM((SLOTS, width, cache), BF16),
            pltpu.VMEM((rows, d), BF16),
            pltpu.VMEM((1, d), BF16),
            pltpu.VMEM((1, d), BF16),
            pltpu.VMEM((2, width), F32),
            pltpu.VMEM((d, width), BF16),
            pltpu.VMEM((width, d), BF16),
            pltpu.VMEM((d, 2 * hidden), BF16),
            pltpu.VMEM((hidden, d), BF16),
            pltpu.VMEM((rows, d), F32),
            pltpu.VMEM((rows, d), F32),
            pltpu.VMEM((rows, width), F32),
            pltpu.VMEM((rows, width), F32),
            pltpu.VMEM((2, 8, cache), F32),
            pltpu.SemaphoreType.DMA((SLOTS,)),
            pltpu.SemaphoreType.DMA((SLOTS,)),
            pltpu.SemaphoreType.DMA((9,)),
            *[pltpu.VMEM((n, size, d), BF16) for size in CHUNKS],
            *[pltpu.VMEM((n, size, d), BF16) for size in CHUNKS],
            pltpu.SemaphoreType.DMA((2, chunks, n - 1)),
            pltpu.SemaphoreType.DMA((2, chunks, n)),
        ]
        return pl.pallas_call(
            functools.partial(kernel, n),
            out_shape=jax.ShapeDtypeStruct((rows, d), BF16),
            in_specs=[pl.BlockSpec(memory_space=pl.ANY)] * 11,
            out_specs=pl.BlockSpec(memory_space=pltpu.VMEM),
            scratch_shapes=scratch,
            compiler_params=pltpu.CompilerParams(collective_id=0, has_side_effects=True, vmem_limit_bytes=65_000_000),
        )(flat(k_cache), flat(v_cache), x, gain_a.reshape(1, d), wq, wo, gain_m.reshape(1, d), w_gate, w_up, w_down, table)

    states, cache, columns, rows_of = P("dp", None), P("dp", None, "tp", None), P(None, "tp"), P("tp", None)
    return jax.shard_map(
        step,
        mesh=mesh,
        in_specs=(states, cache, cache, P(None), columns, rows_of, P(None), columns, columns, rows_of),
        out_specs=states,
        check_vma=False,
    )
```

```python
import functools

import jax
import jax.numpy as jnp
import numpy as np
from jax import lax
from jax.experimental import pallas as pl
from jax.experimental.pallas import tpu as pltpu
from jax.sharding import PartitionSpec as P

HEAD = 64
THETA = 10000
EPS = 1e-6
SLOTS = 8
CHUNKS = ((32, True), (20, True), (8, False), (4, False))
EVENTS = (
    (32, (("project", 0),)),
    (36, (("reduce1", 0),)),
    (40, (("feed", 0),)),
    (44, (("reduce2", 0),)),
    (48, (("finish", 0),)),
    (52, (("project", 1),)),
    (54, (("reduce1", 1),)),
    (58, (("feed", 1),)),
    (60, (("project", 2),)),
    (64, (("project", 3), ("reduce2", 1), ("feed", 2), ("feed", 3), ("finish", 1), ("finish", 2), ("finish", 3))),
)
MESH = pl.DeviceIdType.MESH
F32, BF16 = jnp.float32, jnp.bfloat16


def turn_table(place, heads):
    half = HEAD // 2
    angle = np.float32(place) * np.float32(THETA) ** (-np.arange(half, dtype=np.float32) / np.float32(half))
    angle = angle.astype(np.float32)
    cos, sin = np.cos(angle), np.sin(angle)
    return np.stack([np.tile(np.concatenate([cos, cos]), heads), np.tile(np.concatenate([-sin, sin]), heads)]).astype(np.float32)


def dot(a, b):
    return jnp.dot(a, b, preferred_element_type=F32)


def dot_t(a, b):
    return lax.dot_general(a, b, (((1,), (1,)), ((), ())), preferred_element_type=F32)


def normed(wide, gain):
    return (wide * lax.rsqrt(jnp.mean(wide * wide, -1, keepdims=True) + EPS) * gain).astype(BF16)


def row_of(ref):
    wide = ref[...].astype(F32)
    return jnp.concatenate([wide[i : i + 1, :] for i in range(wide.shape[0])], 1)


def kernel(n, k_hbm, v_hbm, x_hbm, ga_hbm, wq_hbm, wo_hbm, gm_hbm, wg_hbm, wu_hbm, wd_hbm, table_hbm, y_ref, *scratch):
    rows, width, cache = k_hbm.shape
    heads = width // HEAD
    hidden = wg_hbm.shape[1]
    (kbuf, vbuf, x_ref, ga, gm, table, wq, wo, wgu, wd, xf, hf, qf, seen, scores, ksem, vsem, wsem) = scratch[:18]
    chunks = len(CHUNKS)
    send_sem, recv_sem = scratch[18:20]
    rest, bufs = list(scratch[20:]), []
    for _, split in CHUNKS:
        count = 6 if split else 2
        bufs.append(rest[:count])
        rest = rest[count:]
    me = lax.axis_index("tp")
    peers = [lax.rem(me + i, n) for i in range(1, n)]
    if n == 8:
        x, y, core = me // 4, lax.rem(me // 2, 2), lax.rem(me, 2)
        far = [(1, 1, 0), (1, 1, 1), (1, 0, 0), (0, 1, 0), (1, 0, 1), (0, 1, 1), (0, 0, 1)]
        peers = [lax.rem(x + i, 2) * 4 + lax.rem(y + j, 2) * 2 + lax.rem(core + k, 2) for i, j, k in far]

    def kcopy(s):
        slot = lax.rem(s, SLOTS)
        return pltpu.make_async_copy(k_hbm.at[s], kbuf.at[slot], ksem.at[slot])

    def vcopy(s):
        slot = lax.rem(s, SLOTS)
        return pltpu.make_async_copy(v_hbm.at[s], vbuf.at[slot], vsem.at[slot])

    small = [
        pltpu.make_async_copy(src, dst, wsem.at[i])
        for i, (src, dst) in enumerate(
            [
                (x_hbm, x_ref),
                (ga_hbm, ga),
                (wq_hbm, wq),
                (table_hbm, table),
                (wo_hbm, wo),
                (gm_hbm, gm),
                (wg_hbm, wgu.at[:, :hidden]),
                (wu_hbm, wgu.at[:, hidden:]),
                (wd_hbm, wd),
            ]
        )
    ]
    for copy in small[:4]:
        copy.start()
    for s in range(SLOTS):
        kcopy(s).start()
        vcopy(s).start()
    for copy in small[4:]:
        copy.start()

    barrier = pltpu.get_barrier_semaphore()
    for peer in peers:
        pl.semaphore_signal(barrier, inc=1, device_id={"tp": peer}, device_id_type=MESH)

    for copy in small[:2]:
        copy.wait()
    xf[...] = x_ref[...].astype(F32)
    a = normed(xf[...], row_of(ga))
    for copy in small[2:4]:
        copy.wait()
    q = dot(a, wq[...]).astype(BF16).astype(F32)
    half = HEAD // 2
    lane = lax.broadcasted_iota(jnp.int32, q.shape, 1)
    other = jnp.where(lax.rem(lane, HEAD) < half, pltpu.roll(q, width - half, 1), pltpu.roll(q, half, 1))
    qf[...] = (q * table[0:1, :] + other * table[1:2, :]).astype(BF16).astype(F32)

    own = lax.broadcasted_iota(jnp.int32, (8, width), 1) // HEAD == lax.broadcasted_iota(jnp.int32, (8, width), 0)

    def score(s):
        query = jnp.where(own, jnp.broadcast_to(qf[pl.ds(s, 1), :], (8, width)), 0.0).astype(BF16)
        return dot(query, kbuf[lax.rem(s, SLOTS)])

    def attend(s, wide):
        scaled = wide * HEAD**-0.5
        e = jnp.exp(scaled - jnp.max(scaled, -1, keepdims=True))
        weights = (e * (1.0 / jnp.sum(e, -1, keepdims=True))).astype(BF16)
        out = dot_t(weights, vbuf[lax.rem(s, SLOTS)])
        seen[pl.ds(s, 1), :] = jnp.sum(jnp.where(own, out, 0.0), 0, keepdims=True)

    def send(kind, c, i, src, dst):
        return pltpu.make_async_remote_copy(
            src_ref=src,
            dst_ref=dst,
            send_sem=send_sem.at[kind, c, i],
            recv_sem=recv_sem.at[kind, c, me],
            device_id={"tp": peers[i]},
            device_id_type=MESH,
        )

    def arrive(kind, c, buf):
        for peer in peers:
            pltpu.make_async_remote_copy(
                src_ref=buf.at[peer],
                dst_ref=buf.at[peer],
                send_sem=send_sem.at[kind, c, 0],
                recv_sem=recv_sem.at[kind, c, peer],
                device_id={"tp": peer},
                device_id_type=MESH,
            ).wait_recv()

    def total(buf):
        out = buf[0].astype(F32)
        for i in range(1, n):
            out = out + buf[i].astype(F32)
        return out

    def joined(buf):
        return jnp.concatenate([buf[i].astype(F32) for i in range(n)], 1)

    def spread(kind, c, buf):
        return [send(kind, c, i, buf.at[me], buf.at[me]) for i in range(n - 1)]

    def scatter(kind, c, src, dst):
        return [send(kind, c, i, src.at[peers[i]], dst.at[me]) for i in range(n - 1)]

    def start(copies):
        for copy in copies:
            copy.start()

    starts = [sum(size for size, _ in CHUNKS[:c]) for c in range(chunks)]
    parts = [slice(starts[c], starts[c] + CHUNKS[c][0]) for c in range(chunks)]
    tile = x_hbm.shape[1] // n
    mine = pl.ds(pl.multiple_of(me * tile, tile), tile)

    def send_term(half, c, term):
        if CHUNKS[c][1]:
            staged, landed = bufs[c][3 * half], bufs[c][3 * half + 1]
            for i in range(n):
                staged[i] = term[:, i * tile : (i + 1) * tile].astype(BF16)
            start(scatter(2 * half, c, staged, landed))
            landed[me] = staged[me]
        else:
            buf = bufs[c][half]
            buf[me] = term.astype(BF16)
            start(spread(2 * half, c, buf))

    def project(c):
        if c == 0:
            for copy in small[4:]:
                copy.wait()
            pl.semaphore_wait(barrier, n - 1)
        send_term(0, c, dot(seen[parts[c], :].astype(BF16), wo[...]))

    def reduce(half, c):
        landed, whole = bufs[c][3 * half + 1 : 3 * half + 3]
        arrive(2 * half, c, landed)
        before = xf[parts[c], mine] if half == 0 else bufs[c][2][me].astype(F32)
        whole[me] = (before + total(landed)).astype(BF16)
        start(spread(2 * half + 1, c, whole))

    def feed(c):
        if CHUNKS[c][1]:
            arrive(1, c, bufs[c][2])
            h = joined(bufs[c][2])
        else:
            arrive(0, c, bufs[c][0])
            h = (xf[parts[c], :] + total(bufs[c][0])).astype(BF16).astype(F32)
            hf[parts[c], :] = h
        b = normed(h, row_of(gm))
        both = dot(b, wgu[...])
        gate, up = both[:, :hidden], both[:, hidden:]
        product = (gate * (1.0 / (1.0 + jnp.exp(-gate))) * up).astype(BF16)
        send_term(1, c, dot(product, wd[...]))

    def finish(c):
        if CHUNKS[c][1]:
            arrive(3, c, bufs[c][5])
            y_ref[parts[c], :] = joined(bufs[c][5]).astype(BF16)
        else:
            arrive(2, c, bufs[c][1])
            y_ref[parts[c], :] = (hf[parts[c], :] + total(bufs[c][1])).astype(BF16)

    stages = {"project": project, "reduce1": functools.partial(reduce, 0), "feed": feed, "reduce2": functools.partial(reduce, 1), "finish": finish}

    kcopy(0).wait()
    scores[0] = score(0)
    kcopy(SLOTS).start()

    def step(s, _):
        kcopy(s + 1).wait()
        vcopy(s).wait()
        wide = scores[lax.rem(s, 2)]
        scores[lax.rem(s + 1, 2)] = score(s + 1)
        attend(s, wide)

        @pl.when(s + 1 + SLOTS < rows)
        def _():
            kcopy(s + 1 + SLOTS).start()

        @pl.when(s + SLOTS < rows)
        def _():
            vcopy(s + SLOTS).start()

        for row, names in EVENTS:
            if row < rows:

                @pl.when(s == row - 1)
                def _():
                    for name, c in names:
                        stages[name](c)

        return 0

    lax.fori_loop(0, rows - 1, step, 0)
    vcopy(rows - 1).wait()
    attend(rows - 1, scores[(rows - 1) % 2])
    for row, names in EVENTS:
        if row == rows:
            for name, c in names:
                stages[name](c)

    for c in range(chunks):
        for half in range(2):
            if CHUNKS[c][1]:
                copies = scatter(2 * half, c, *bufs[c][3 * half : 3 * half + 2]) + spread(2 * half + 1, c, bufs[c][3 * half + 2])
            else:
                copies = spread(2 * half, c, bufs[c][half])
            for copy in copies:
                copy.wait_send()


def solution(mesh):
    n = mesh.shape["tp"]

    def step(x, k_cache, v_cache, gain_a, wq, wo, gain_m, w_gate, w_up, w_down):
        rows, cache, heads, head = k_cache.shape
        d, width, hidden = x.shape[1], heads * head, w_gate.shape[1]
        flat = lambda t: t.transpose(0, 2, 3, 1).reshape(rows, width, cache)
        table = jnp.asarray(turn_table(cache - 1, heads))
        chunks = len(CHUNKS)
        scratch = [
            pltpu.VMEM((SLOTS, width, cache), BF16),
            pltpu.VMEM((SLOTS, width, cache), BF16),
            pltpu.VMEM((rows, d), BF16),
            pltpu.VMEM((d // 128, 128), BF16),
            pltpu.VMEM((d // 128, 128), BF16),
            pltpu.VMEM((2, width), F32),
            pltpu.VMEM((d, width), BF16),
            pltpu.VMEM((width, d), BF16),
            pltpu.VMEM((d, 2 * hidden), BF16),
            pltpu.VMEM((hidden, d), BF16),
            pltpu.VMEM((rows, d), F32),
            pltpu.VMEM((rows, d), F32),
            pltpu.VMEM((rows, width), F32),
            pltpu.VMEM((rows, width), F32),
            pltpu.VMEM((2, 8, cache), F32),
            pltpu.SemaphoreType.DMA((SLOTS,)),
            pltpu.SemaphoreType.DMA((SLOTS,)),
            pltpu.SemaphoreType.DMA((9,)),
            pltpu.SemaphoreType.DMA((4, chunks, n - 1)),
            pltpu.SemaphoreType.DMA((4, chunks, n)),
        ]
        for size, split in CHUNKS:
            scratch += [pltpu.VMEM((n, size, d // n), BF16)] * 6 if split else [pltpu.VMEM((n, size, d), BF16)] * 2
        return pl.pallas_call(
            functools.partial(kernel, n),
            out_shape=pltpu.VMEM((rows, d), BF16),
            in_specs=[pl.BlockSpec(memory_space=pl.ANY)] * 11,
            out_specs=pl.BlockSpec(memory_space=pltpu.VMEM),
            scratch_shapes=scratch,
            compiler_params=pltpu.CompilerParams(collective_id=0, has_side_effects=True, vmem_limit_bytes=58_000_000),
        )(flat(k_cache), flat(v_cache), x, gain_a.reshape(d // 128, 128), wq, wo, gain_m.reshape(d // 128, 128), w_gate, w_up, w_down, table)

    states, cache, columns, rows_of = P("dp", None), P("dp", None, "tp", None), P(None, "tp"), P("tp", None)
    return jax.shard_map(
        step,
        mesh=mesh,
        in_specs=(states, cache, cache, P(None), columns, rows_of, P(None), columns, columns, rows_of),
        out_specs=states,
        check_vma=False,
    )
```

```python
import functools

import jax
import jax.numpy as jnp
import numpy as np
from jax import lax
from jax.experimental import pallas as pl
from jax.experimental.pallas import tpu as pltpu
from jax.sharding import PartitionSpec as P

HEAD = 64
THETA = 10000
EPS = 1e-6
SLOTS = 8
CHUNKS = ((32, True), (20, True), (8, False), (4, False))
EVENTS = (
    (32, (("project", 0),)),
    (36, (("reduce1", 0),)),
    (40, (("feed", 0),)),
    (44, (("reduce2", 0),)),
    (48, (("finish", 0),)),
    (52, (("project", 1),)),
    (54, (("reduce1", 1),)),
    (58, (("feed", 1),)),
    (60, (("project", 2),)),
    (64, (("project", 3), ("reduce2", 1), ("feed", 2), ("feed", 3), ("finish", 1), ("finish", 2), ("finish", 3))),
)
PIECES = 4
MESH = pl.DeviceIdType.MESH
F32, BF16 = jnp.float32, jnp.bfloat16


def turn_table(place, heads):
    half = HEAD // 2
    angle = np.float32(place) * np.float32(THETA) ** (-np.arange(half, dtype=np.float32) / np.float32(half))
    angle = angle.astype(np.float32)
    cos, sin = np.cos(angle), np.sin(angle)
    return np.stack([np.tile(np.concatenate([cos, cos]), heads), np.tile(np.concatenate([-sin, sin]), heads)]).astype(np.float32)


def dot(a, b):
    return jnp.dot(a, b, preferred_element_type=F32)


def dot_t(a, b):
    return lax.dot_general(a, b, (((1,), (1,)), ((), ())), preferred_element_type=F32)


def normed(wide, gain):
    return (wide * lax.rsqrt(jnp.mean(wide * wide, -1, keepdims=True) + EPS) * gain).astype(BF16)


def row_of(ref):
    wide = ref[...].astype(F32)
    return jnp.concatenate([wide[i : i + 1, :] for i in range(wide.shape[0])], 1)


def kernel(n, k_hbm, v_hbm, x_hbm, ga_hbm, wq_hbm, wo_hbm, gm_hbm, wg_hbm, wu_hbm, wd_hbm, table_hbm, y_ref, *scratch):
    rows, width, cache = k_hbm.shape
    heads = width // HEAD
    hidden = wg_hbm.shape[1]
    (kbuf, vbuf, x_ref, ga, gm, table, wq, wo, wgu, wd, xf, hf, qf, seen, scores, ksem, vsem, wsem) = scratch[:18]
    chunks = len(CHUNKS)
    send_sem, recv_sem = scratch[18:20]
    last_sem = scratch[20]
    rest, bufs, slots, used = list(scratch[21:]), [], [], 0
    for _, split in CHUNKS:
        kinds = range(4) if split else (0, 2)
        slots.append({kind: used + i for i, kind in enumerate(kinds)})
        used += len(kinds)
        count = 6 if split else 2
        bufs.append(rest[:count])
        rest = rest[count:]
    me = lax.axis_index("tp")
    peers = [lax.rem(me + i, n) for i in range(1, n)]
    if n == 8:
        x, y, core = me // 4, lax.rem(me // 2, 2), lax.rem(me, 2)
        far = [(1, 1, 0), (1, 1, 1), (1, 0, 0), (0, 1, 0), (1, 0, 1), (0, 1, 1), (0, 0, 1)]
        peers = [lax.rem(x + i, 2) * 4 + lax.rem(y + j, 2) * 2 + lax.rem(core + k, 2) for i, j, k in far]

    def kcopy(s):
        slot = lax.rem(s, SLOTS)
        return pltpu.make_async_copy(k_hbm.at[s], kbuf.at[slot], ksem.at[slot])

    def vcopy(s):
        slot = lax.rem(s, SLOTS)
        return pltpu.make_async_copy(v_hbm.at[s], vbuf.at[slot], vsem.at[slot])

    def vpieces():
        size = cache // PIECES
        slot = (rows - 1) % SLOTS
        return [
            pltpu.make_async_copy(v_hbm.at[rows - 1, :, pl.ds(i * size, size)], vbuf.at[slot, :, pl.ds(i * size, size)], last_sem.at[i])
            for i in range(PIECES)
        ]

    small = [
        pltpu.make_async_copy(src, dst, wsem.at[i])
        for i, (src, dst) in enumerate(
            [
                (x_hbm, x_ref),
                (ga_hbm, ga),
                (wq_hbm, wq),
                (table_hbm, table),
                (wo_hbm, wo),
                (gm_hbm, gm),
                (wg_hbm, wgu.at[:, :hidden]),
                (wu_hbm, wgu.at[:, hidden:]),
                (wd_hbm, wd),
            ]
        )
    ]
    for copy in small[:4]:
        copy.start()
    for s in range(SLOTS):
        kcopy(s).start()
        vcopy(s).start()
    for copy in small[4:]:
        copy.start()

    barrier = pltpu.get_barrier_semaphore()
    for peer in peers:
        pl.semaphore_signal(barrier, inc=1, device_id={"tp": peer}, device_id_type=MESH)

    for copy in small[:2]:
        copy.wait()
    xf[...] = x_ref[...].astype(F32)
    a = normed(xf[...], row_of(ga))
    for copy in small[2:4]:
        copy.wait()
    q = dot(a, wq[...]).astype(BF16).astype(F32)
    half = HEAD // 2
    lane = lax.broadcasted_iota(jnp.int32, q.shape, 1)
    other = jnp.where(lax.rem(lane, HEAD) < half, pltpu.roll(q, width - half, 1), pltpu.roll(q, half, 1))
    qf[...] = (q * table[0:1, :] + other * table[1:2, :]).astype(BF16).astype(F32)

    own = lax.broadcasted_iota(jnp.int32, (8, width), 1) // HEAD == lax.broadcasted_iota(jnp.int32, (8, width), 0)

    def score(s):
        query = jnp.where(own, jnp.broadcast_to(qf[pl.ds(s, 1), :], (8, width)), 0.0).astype(BF16)
        return dot(query, kbuf[lax.rem(s, SLOTS)])

    def weigh(wide):
        scaled = wide * HEAD**-0.5
        e = jnp.exp(scaled - jnp.max(scaled, -1, keepdims=True))
        return (e * (1.0 / jnp.sum(e, -1, keepdims=True))).astype(BF16)

    def keep(s, out):
        seen[pl.ds(s, 1), :] = jnp.sum(jnp.where(own, out, 0.0), 0, keepdims=True)

    def attend(s, wide):
        keep(s, dot_t(weigh(wide), vbuf[lax.rem(s, SLOTS)]))

    def send(kind, c, i, src, dst):
        return pltpu.make_async_remote_copy(
            src_ref=src,
            dst_ref=dst,
            send_sem=send_sem.at[slots[c][kind]],
            recv_sem=recv_sem.at[slots[c][kind]],
            device_id={"tp": peers[i]},
            device_id_type=MESH,
        )

    def others(kind, c, src, dst):
        return pltpu.make_async_remote_copy(
            src_ref=src.at[pl.ds(0, n - 1)],
            dst_ref=dst.at[pl.ds(0, n - 1)],
            send_sem=send_sem.at[slots[c][kind]],
            recv_sem=recv_sem.at[slots[c][kind]],
            device_id={"tp": peers[0]},
            device_id_type=MESH,
        )

    def arrive(kind, c, buf):
        others(kind, c, buf, buf).wait_recv()

    def total(buf):
        out = buf[0].astype(F32)
        for i in range(1, n):
            out = out + buf[i].astype(F32)
        return out

    def joined(buf):
        return jnp.concatenate([buf[i].astype(F32) for i in range(n)], 1)

    def spread(kind, c, buf):
        return [send(kind, c, i, buf.at[me], buf.at[me]) for i in range(n - 1)]

    def scatter(kind, c, src, dst):
        return [send(kind, c, i, src.at[peers[i]], dst.at[me]) for i in range(n - 1)]

    def start(copies):
        for copy in copies:
            copy.start()

    starts = [sum(size for size, _ in CHUNKS[:c]) for c in range(chunks)]
    parts = [slice(starts[c], starts[c] + CHUNKS[c][0]) for c in range(chunks)]
    tile = x_hbm.shape[1] // n
    mine = pl.ds(pl.multiple_of(me * tile, tile), tile)

    def send_term(half, c, term):
        if CHUNKS[c][1]:
            staged, landed = bufs[c][3 * half], bufs[c][3 * half + 1]
            for i in range(n):
                staged[i] = term[:, i * tile : (i + 1) * tile].astype(BF16)
            start(scatter(2 * half, c, staged, landed))
            landed[me] = staged[me]
        else:
            buf = bufs[c][half]
            buf[me] = term.astype(BF16)
            start(spread(2 * half, c, buf))

    def project(c):
        if c == 0:
            for copy in small[4:]:
                copy.wait()
            pl.semaphore_wait(barrier, n - 1)
        send_term(0, c, dot(seen[parts[c], :].astype(BF16), wo[...]))

    def reduce(half, c):
        landed, whole = bufs[c][3 * half + 1 : 3 * half + 3]
        arrive(2 * half, c, landed)
        before = xf[parts[c], mine] if half == 0 else bufs[c][2][me].astype(F32)
        whole[me] = (before + total(landed)).astype(BF16)
        start(spread(2 * half + 1, c, whole))

    def states(c):
        if CHUNKS[c][1]:
            arrive(1, c, bufs[c][2])
            return joined(bufs[c][2])
        arrive(0, c, bufs[c][0])
        h = (xf[parts[c], :] + total(bufs[c][0])).astype(BF16).astype(F32)
        hf[parts[c], :] = h
        return h

    def feed(*group):
        h = jnp.concatenate([states(c) for c in group], 0)
        b = normed(h, row_of(gm))
        both = dot(b, wgu[...])
        gate, up = both[:, :hidden], both[:, hidden:]
        product = (gate * (1.0 / (1.0 + jnp.exp(-gate))) * up).astype(BF16)
        term, at = dot(product, wd[...]), 0
        for c in group:
            send_term(1, c, term[at : at + CHUNKS[c][0], :])
            at += CHUNKS[c][0]

    def finish(c):
        if CHUNKS[c][1]:
            arrive(3, c, bufs[c][5])
            y_ref[parts[c], :] = joined(bufs[c][5]).astype(BF16)
        else:
            arrive(2, c, bufs[c][1])
            y_ref[parts[c], :] = (hf[parts[c], :] + total(bufs[c][1])).astype(BF16)

    stages = {"project": project, "reduce1": functools.partial(reduce, 0), "feed": feed, "reduce2": functools.partial(reduce, 1), "finish": finish}

    kcopy(0).wait()
    scores[0] = score(0)
    kcopy(SLOTS).start()

    def step(s, _):
        kcopy(s + 1).wait()
        vcopy(s).wait()
        wide = scores[lax.rem(s, 2)]
        scores[lax.rem(s + 1, 2)] = score(s + 1)
        attend(s, wide)

        @pl.when(s + 1 + SLOTS < rows)
        def _():
            kcopy(s + 1 + SLOTS).start()

        @pl.when(s + SLOTS < rows - 1)
        def _():
            vcopy(s + SLOTS).start()

        @pl.when(s + SLOTS == rows - 1)
        def _():
            start(vpieces())

        for row, names in EVENTS:
            if row < rows:

                @pl.when(s == row - 1)
                def _():
                    for name, *group in names:
                        stages[name](*group)

        return 0

    lax.fori_loop(0, rows - 1, step, 0)
    weights = weigh(scores[(rows - 1) % 2])
    size = cache // PIECES
    out = jnp.zeros((8, width), F32)
    for i, copy in enumerate(vpieces()):
        copy.wait()
        out = out + dot_t(weights[:, i * size : (i + 1) * size], vbuf[(rows - 1) % SLOTS, :, i * size : (i + 1) * size])
    keep(rows - 1, out)
    for row, names in EVENTS:
        if row == rows:
            for name, *group in names:
                stages[name](*group)

    for c in range(chunks):
        for half in range(2):
            if CHUNKS[c][1]:
                others(2 * half, c, bufs[c][3 * half], bufs[c][3 * half + 1]).wait_send()
                others(2 * half + 1, c, bufs[c][3 * half + 2], bufs[c][3 * half + 2]).wait_send()
            else:
                others(2 * half, c, bufs[c][half], bufs[c][half]).wait_send()


def solution(mesh):
    n = mesh.shape["tp"]

    def step(x, k_cache, v_cache, gain_a, wq, wo, gain_m, w_gate, w_up, w_down):
        rows, cache, heads, head = k_cache.shape
        d, width, hidden = x.shape[1], heads * head, w_gate.shape[1]
        flat = lambda t: t.transpose(0, 2, 3, 1).reshape(rows, width, cache)
        table = jnp.asarray(turn_table(cache - 1, heads))
        exchanges = sum(4 if split else 2 for _, split in CHUNKS)
        scratch = [
            pltpu.VMEM((SLOTS, width, cache), BF16),
            pltpu.VMEM((SLOTS, width, cache), BF16),
            pltpu.VMEM((rows, d), BF16),
            pltpu.VMEM((d // 128, 128), BF16),
            pltpu.VMEM((d // 128, 128), BF16),
            pltpu.VMEM((2, width), F32),
            pltpu.VMEM((d, width), BF16),
            pltpu.VMEM((width, d), BF16),
            pltpu.VMEM((d, 2 * hidden), BF16),
            pltpu.VMEM((hidden, d), BF16),
            pltpu.VMEM((rows, d), F32),
            pltpu.VMEM((rows, d), F32),
            pltpu.VMEM((rows, width), F32),
            pltpu.VMEM((rows, width), F32),
            pltpu.VMEM((2, 8, cache), F32),
            pltpu.SemaphoreType.DMA((SLOTS,)),
            pltpu.SemaphoreType.DMA((SLOTS,)),
            pltpu.SemaphoreType.DMA((9,)),
            pltpu.SemaphoreType.DMA((exchanges,)),
            pltpu.SemaphoreType.DMA((exchanges,)),
            pltpu.SemaphoreType.DMA((PIECES,)),
        ]
        for size, split in CHUNKS:
            scratch += [pltpu.VMEM((n, size, d // n), BF16)] * 6 if split else [pltpu.VMEM((n, size, d), BF16)] * 2
        return pl.pallas_call(
            functools.partial(kernel, n),
            out_shape=pltpu.VMEM((rows, d), BF16),
            in_specs=[pl.BlockSpec(memory_space=pl.ANY)] * 11,
            out_specs=pl.BlockSpec(memory_space=pltpu.VMEM),
            scratch_shapes=scratch,
            compiler_params=pltpu.CompilerParams(collective_id=0, has_side_effects=True, vmem_limit_bytes=58_000_000),
        )(flat(k_cache), flat(v_cache), x, gain_a.reshape(d // 128, 128), wq, wo, gain_m.reshape(d // 128, 128), w_gate, w_up, w_down, table)

    states, cache, columns, rows_of = P("dp", None), P("dp", None, "tp", None), P(None, "tp"), P("tp", None)
    return jax.shard_map(
        step,
        mesh=mesh,
        in_specs=(states, cache, cache, P(None), columns, rows_of, P(None), columns, columns, rows_of),
        out_specs=states,
        check_vma=False,
    )
```

```python
import functools

import jax
import jax.numpy as jnp
import numpy as np
from jax import lax
from jax.experimental import pallas as pl
from jax.experimental.pallas import tpu as pltpu
from jax.sharding import PartitionSpec as P

HEAD = 64
THETA = 10000
EPS = 1e-6
SLOTS = 8
CHUNKS = ((40, True, True), (16, True, True), (4, False, False), (4, False, False))
EVENTS = (
    (40, (("project", 0),)),
    (44, (("reduce1", 0),)),
    (48, (("feed", 0),)),
    (52, (("reduce2", 0),)),
    (56, (("project", 1),)),
    (57, (("finish", 0),)),
    (60, (("project", 2), ("reduce1", 1))),
    (64, (("project", 3), ("feed", 1, 2), ("feed", 3), ("reduce2", 1), ("finish", 1), ("finish", 2), ("finish", 3))),
)
PIECES = 4
MESH = pl.DeviceIdType.MESH
F32, BF16 = jnp.float32, jnp.bfloat16


def turn_table(place, heads):
    half = HEAD // 2
    angle = np.float32(place) * np.float32(THETA) ** (-np.arange(half, dtype=np.float32) / np.float32(half))
    angle = angle.astype(np.float32)
    cos, sin = np.cos(angle), np.sin(angle)
    return np.stack([np.tile(np.concatenate([cos, cos]), heads), np.tile(np.concatenate([-sin, sin]), heads)]).astype(np.float32)


def dot(a, b):
    return jnp.dot(a, b, preferred_element_type=F32)


def dot_t(a, b):
    return lax.dot_general(a, b, (((1,), (1,)), ((), ())), preferred_element_type=F32)


def normed(wide, gain):
    return (wide * lax.rsqrt(jnp.mean(wide * wide, -1, keepdims=True) + EPS) * gain).astype(BF16)


def row_of(ref):
    wide = ref[...].astype(F32)
    return jnp.concatenate([wide[i : i + 1, :] for i in range(wide.shape[0])], 1)


def kernel(n, k_hbm, v_hbm, x_hbm, ga_hbm, wq_hbm, wo_hbm, gm_hbm, wg_hbm, wu_hbm, wd_hbm, table_hbm, y_ref, *scratch):
    rows, width, cache = k_hbm.shape
    heads = width // HEAD
    hidden = wg_hbm.shape[1]
    (kbuf, vbuf, x_ref, ga, gm, table, wq, wo, wgu, wd, xf, hf, qf, seen, scores, ksem, vsem, wsem) = scratch[:18]
    chunks = len(CHUNKS)
    send_sem, recv_sem = scratch[18:20]
    last_sem = scratch[20]
    rest, bufs, slots, used = list(scratch[21:]), [], [], 0
    for _, *splits in CHUNKS:
        bufs.append([])
        slots.append({})
        for half, split in enumerate(splits):
            bufs[-1].append(rest[: 3 if split else 1])
            rest = rest[3 if split else 1 :]
            for kind in (2 * half, 2 * half + 1) if split else (2 * half,):
                slots[-1][kind] = used
                used += 1
    me = lax.axis_index("tp")
    peers = [lax.rem(me + i, n) for i in range(1, n)]
    if n == 8:
        x, y, core = me // 4, lax.rem(me // 2, 2), lax.rem(me, 2)
        far = [(1, 1, 0), (1, 1, 1), (1, 0, 0), (0, 1, 0), (1, 0, 1), (0, 1, 1), (0, 0, 1)]
        peers = [lax.rem(x + i, 2) * 4 + lax.rem(y + j, 2) * 2 + lax.rem(core + k, 2) for i, j, k in far]

    def kcopy(s):
        slot = lax.rem(s, SLOTS)
        return pltpu.make_async_copy(k_hbm.at[s], kbuf.at[slot], ksem.at[slot])

    def vcopy(s):
        slot = lax.rem(s, SLOTS)
        return pltpu.make_async_copy(v_hbm.at[s], vbuf.at[slot], vsem.at[slot])

    def vpieces():
        size = cache // PIECES
        slot = (rows - 1) % SLOTS
        return [
            pltpu.make_async_copy(v_hbm.at[rows - 1, :, pl.ds(i * size, size)], vbuf.at[slot, :, pl.ds(i * size, size)], last_sem.at[i])
            for i in range(PIECES)
        ]

    small = [
        pltpu.make_async_copy(src, dst, wsem.at[i])
        for i, (src, dst) in enumerate(
            [
                (x_hbm, x_ref),
                (ga_hbm, ga),
                (wq_hbm, wq),
                (table_hbm, table),
                (wo_hbm, wo),
                (gm_hbm, gm),
                (wg_hbm, wgu.at[:, :hidden]),
                (wu_hbm, wgu.at[:, hidden:]),
                (wd_hbm, wd),
            ]
        )
    ]
    for copy in small[:4]:
        copy.start()
    for s in range(SLOTS):
        kcopy(s).start()
        vcopy(s).start()
    for copy in small[4:]:
        copy.start()

    barrier = pltpu.get_barrier_semaphore()
    for peer in peers:
        pl.semaphore_signal(barrier, inc=1, device_id={"tp": peer}, device_id_type=MESH)

    for copy in small[:2]:
        copy.wait()
    xf[...] = x_ref[...].astype(F32)
    a = normed(xf[...], row_of(ga))
    for copy in small[2:4]:
        copy.wait()
    q = dot(a, wq[...]).astype(BF16).astype(F32)
    half = HEAD // 2
    lane = lax.broadcasted_iota(jnp.int32, q.shape, 1)
    other = jnp.where(lax.rem(lane, HEAD) < half, pltpu.roll(q, width - half, 1), pltpu.roll(q, half, 1))
    qf[...] = (q * table[0:1, :] + other * table[1:2, :]).astype(BF16).astype(F32)

    own = lax.broadcasted_iota(jnp.int32, (8, width), 1) // HEAD == lax.broadcasted_iota(jnp.int32, (8, width), 0)

    def score(s):
        query = jnp.where(own, jnp.broadcast_to(qf[pl.ds(s, 1), :], (8, width)), 0.0).astype(BF16)
        return dot(query, kbuf[lax.rem(s, SLOTS)])

    def weigh(wide):
        scaled = wide * HEAD**-0.5
        e = jnp.exp(scaled - jnp.max(scaled, -1, keepdims=True))
        return (e * (1.0 / jnp.sum(e, -1, keepdims=True))).astype(BF16)

    def keep(s, out):
        seen[pl.ds(s, 1), :] = jnp.sum(jnp.where(own, out, 0.0), 0, keepdims=True)

    def attend(s, wide):
        keep(s, dot_t(weigh(wide), vbuf[lax.rem(s, SLOTS)]))

    def send(kind, c, i, src, dst):
        return pltpu.make_async_remote_copy(
            src_ref=src,
            dst_ref=dst,
            send_sem=send_sem.at[slots[c][kind]],
            recv_sem=recv_sem.at[slots[c][kind]],
            device_id={"tp": peers[i]},
            device_id_type=MESH,
        )

    def others(kind, c, src, dst):
        return pltpu.make_async_remote_copy(
            src_ref=src.at[pl.ds(0, n - 1)],
            dst_ref=dst.at[pl.ds(0, n - 1)],
            send_sem=send_sem.at[slots[c][kind]],
            recv_sem=recv_sem.at[slots[c][kind]],
            device_id={"tp": peers[0]},
            device_id_type=MESH,
        )

    def arrive(kind, c, buf):
        others(kind, c, buf, buf).wait_recv()

    def total(buf):
        out = buf[0].astype(F32)
        for i in range(1, n):
            out = out + buf[i].astype(F32)
        return out

    def joined(buf):
        return jnp.concatenate([buf[i].astype(F32) for i in range(n)], 1)

    def spread(kind, c, buf):
        return [send(kind, c, i, buf.at[me], buf.at[me]) for i in range(n - 1)]

    def scatter(kind, c, src, dst):
        return [send(kind, c, i, src.at[peers[i]], dst.at[me]) for i in range(n - 1)]

    def start(copies):
        for copy in copies:
            copy.start()

    starts = [sum(chunk[0] for chunk in CHUNKS[:c]) for c in range(chunks)]
    parts = [slice(starts[c], starts[c] + CHUNKS[c][0]) for c in range(chunks)]
    tile = x_hbm.shape[1] // n
    mine = pl.ds(pl.multiple_of(me * tile, tile), tile)

    def send_term(half, c, term):
        if CHUNKS[c][1 + half]:
            staged, landed, _ = bufs[c][half]
            for i in range(n):
                staged[i] = term[:, i * tile : (i + 1) * tile].astype(BF16)
            start(scatter(2 * half, c, staged, landed))
            landed[me] = staged[me]
        else:
            (buf,) = bufs[c][half]
            buf[me] = term.astype(BF16)
            start(spread(2 * half, c, buf))

    def project(c):
        if c == 0:
            for copy in small[4:]:
                copy.wait()
            pl.semaphore_wait(barrier, n - 1)
        send_term(0, c, dot(seen[parts[c], :].astype(BF16), wo[...]))

    def reduce(half, c):
        _, landed, whole = bufs[c][half]
        arrive(2 * half, c, landed)
        if half == 0:
            before = xf[parts[c], mine]
        elif CHUNKS[c][1]:
            before = bufs[c][0][2][me].astype(F32)
        else:
            before = hf[parts[c], mine]
        whole[me] = (before + total(landed)).astype(BF16)
        start(spread(2 * half + 1, c, whole))

    def states(c):
        if CHUNKS[c][1]:
            arrive(1, c, bufs[c][0][2])
            return joined(bufs[c][0][2])
        (buf,) = bufs[c][0]
        arrive(0, c, buf)
        h = (xf[parts[c], :] + total(buf)).astype(BF16).astype(F32)
        hf[parts[c], :] = h
        return h

    def feed(*group):
        h = jnp.concatenate([states(c) for c in group], 0)
        b = normed(h, row_of(gm))
        both = dot(b, wgu[...])
        gate, up = both[:, :hidden], both[:, hidden:]
        product = (gate * (1.0 / (1.0 + jnp.exp(-gate))) * up).astype(BF16)
        term, at = dot(product, wd[...]), 0
        for c in group:
            send_term(1, c, term[at : at + CHUNKS[c][0], :])
            at += CHUNKS[c][0]

    def finish(c):
        if CHUNKS[c][2]:
            arrive(3, c, bufs[c][1][2])
            y_ref[parts[c], :] = joined(bufs[c][1][2]).astype(BF16)
        else:
            (buf,) = bufs[c][1]
            arrive(2, c, buf)
            y_ref[parts[c], :] = (hf[parts[c], :] + total(buf)).astype(BF16)

    stages = {"project": project, "reduce1": functools.partial(reduce, 0), "feed": feed, "reduce2": functools.partial(reduce, 1), "finish": finish}

    kcopy(0).wait()
    scores[0] = score(0)
    kcopy(SLOTS).start()

    def step(s, _):
        kcopy(s + 1).wait()
        vcopy(s).wait()
        wide = scores[lax.rem(s, 2)]
        scores[lax.rem(s + 1, 2)] = score(s + 1)
        attend(s, wide)

        @pl.when(s + 1 + SLOTS < rows)
        def _():
            kcopy(s + 1 + SLOTS).start()

        @pl.when(s + SLOTS < rows - 1)
        def _():
            vcopy(s + SLOTS).start()

        @pl.when(s + SLOTS == rows - 1)
        def _():
            start(vpieces())

        for row, names in EVENTS:
            if row < rows:

                @pl.when(s == row - 1)
                def _():
                    for name, *group in names:
                        stages[name](*group)

        return 0

    lax.fori_loop(0, rows - 1, step, 0)
    weights = weigh(scores[(rows - 1) % 2])
    size = cache // PIECES
    out = jnp.zeros((8, width), F32)
    for i, copy in enumerate(vpieces()):
        copy.wait()
        out = out + dot_t(weights[:, i * size : (i + 1) * size], vbuf[(rows - 1) % SLOTS, :, i * size : (i + 1) * size])
    keep(rows - 1, out)
    for row, names in EVENTS:
        if row == rows:
            for name, *group in names:
                stages[name](*group)

    for c in range(chunks):
        for half in range(2):
            own_buf, *more = bufs[c][half]
            others(2 * half, c, own_buf, own_buf).wait_send()
            if more:
                others(2 * half + 1, c, more[1], more[1]).wait_send()


def solution(mesh):
    n = mesh.shape["tp"]

    def step(x, k_cache, v_cache, gain_a, wq, wo, gain_m, w_gate, w_up, w_down):
        rows, cache, heads, head = k_cache.shape
        d, width, hidden = x.shape[1], heads * head, w_gate.shape[1]
        flat = lambda t: t.transpose(0, 2, 3, 1).reshape(rows, width, cache)
        table = jnp.asarray(turn_table(cache - 1, heads))
        exchanges = sum(2 if split else 1 for _, *splits in CHUNKS for split in splits)
        scratch = [
            pltpu.VMEM((SLOTS, width, cache), BF16),
            pltpu.VMEM((SLOTS, width, cache), BF16),
            pltpu.VMEM((rows, d), BF16),
            pltpu.VMEM((d // 128, 128), BF16),
            pltpu.VMEM((d // 128, 128), BF16),
            pltpu.VMEM((2, width), F32),
            pltpu.VMEM((d, width), BF16),
            pltpu.VMEM((width, d), BF16),
            pltpu.VMEM((d, 2 * hidden), BF16),
            pltpu.VMEM((hidden, d), BF16),
            pltpu.VMEM((rows, d), F32),
            pltpu.VMEM((rows, d), F32),
            pltpu.VMEM((rows, width), F32),
            pltpu.VMEM((rows, width), F32),
            pltpu.VMEM((2, 8, cache), F32),
            pltpu.SemaphoreType.DMA((SLOTS,)),
            pltpu.SemaphoreType.DMA((SLOTS,)),
            pltpu.SemaphoreType.DMA((9,)),
            pltpu.SemaphoreType.DMA((exchanges,)),
            pltpu.SemaphoreType.DMA((exchanges,)),
            pltpu.SemaphoreType.DMA((PIECES,)),
        ]
        for size, *splits in CHUNKS:
            for split in splits:
                scratch += [pltpu.VMEM((n, size, d // n), BF16)] * 3 if split else [pltpu.VMEM((n, size, d), BF16)]
        return pl.pallas_call(
            functools.partial(kernel, n),
            out_shape=pltpu.VMEM((rows, d), BF16),
            in_specs=[pl.BlockSpec(memory_space=pl.ANY)] * 11,
            out_specs=pl.BlockSpec(memory_space=pltpu.VMEM),
            scratch_shapes=scratch,
            compiler_params=pltpu.CompilerParams(collective_id=0, has_side_effects=True, vmem_limit_bytes=58_000_000),
        )(flat(k_cache), flat(v_cache), x, gain_a.reshape(d // 128, 128), wq, wo, gain_m.reshape(d // 128, 128), w_gate, w_up, w_down, table)

    states, cache, columns, rows_of = P("dp", None), P("dp", None, "tp", None), P(None, "tp"), P("tp", None)
    return jax.shard_map(
        step,
        mesh=mesh,
        in_specs=(states, cache, cache, P(None), columns, rows_of, P(None), columns, columns, rows_of),
        out_specs=states,
        check_vma=False,
    )
```

```python
import functools

import jax
import jax.numpy as jnp
import numpy as np
from jax import lax
from jax.experimental import pallas as pl
from jax.experimental.pallas import tpu as pltpu
from jax.sharding import PartitionSpec as P

HEAD = 64
THETA = 10000
EPS = 1e-6
SLOTS = 8
CHUNKS = ((40, True, True), (16, True, True), (4, False, False), (4, False, False))
EVENTS = (
    (40, (("project", 0),)),
    (44, (("reduce1", 0),)),
    (48, (("feed", 0),)),
    (52, (("reduce2", 0),)),
    (56, (("project", 1),)),
    (57, (("finish", 0),)),
    (60, (("project", 2), ("reduce1", 1))),
    (64, (("project", 3), ("feed", 1, 2), ("feed", 3), ("reduce2", 1), ("finish", 1), ("finish", 2), ("finish", 3))),
)
PIECES = 1
MESH = pl.DeviceIdType.MESH
F32, BF16 = jnp.float32, jnp.bfloat16


def turn_table(place, heads):
    half = HEAD // 2
    angle = np.float32(place) * np.float32(THETA) ** (-np.arange(half, dtype=np.float32) / np.float32(half))
    angle = angle.astype(np.float32)
    cos, sin = np.cos(angle), np.sin(angle)
    return np.stack([np.tile(np.concatenate([cos, cos]), heads), np.tile(np.concatenate([-sin, sin]), heads)]).astype(np.float32)


def dot(a, b):
    return jnp.dot(a, b, preferred_element_type=F32)


def dot_t(a, b):
    return lax.dot_general(a, b, (((1,), (1,)), ((), ())), preferred_element_type=F32)


def normed(wide, gain):
    return (wide * lax.rsqrt(jnp.mean(wide * wide, -1, keepdims=True) + EPS) * gain).astype(BF16)


def row_of(ref):
    wide = ref[...].astype(F32)
    return jnp.concatenate([wide[i : i + 1, :] for i in range(wide.shape[0])], 1)


def kernel(n, k_hbm, v_hbm, x_hbm, ga_hbm, wq_hbm, wo_hbm, gm_hbm, wg_hbm, wu_hbm, wd_hbm, table_hbm, y_ref, *scratch):
    rows, width, cache = k_hbm.shape
    heads = width // HEAD
    hidden = wg_hbm.shape[1]
    (kbuf, vbuf, x_ref, ga, gm, table, wq, wo, wgu, wd, xf, hf, qf, seen, scores, ksem, vsem, wsem) = scratch[:18]
    chunks = len(CHUNKS)
    send_sem, recv_sem = scratch[18:20]
    last_sem = scratch[20]
    rest, bufs, slots, used = list(scratch[21:]), [], [], 0
    for _, *splits in CHUNKS:
        bufs.append([])
        slots.append({})
        for half, split in enumerate(splits):
            bufs[-1].append(rest[: 3 if split else 1])
            rest = rest[3 if split else 1 :]
            for kind in (2 * half, 2 * half + 1) if split else (2 * half,):
                slots[-1][kind] = used
                used += 1
    me = lax.axis_index("tp")
    peers = [lax.rem(me + i, n) for i in range(1, n)]
    if n == 8:
        x, y, core = me // 4, lax.rem(me // 2, 2), lax.rem(me, 2)
        far = [(1, 1, 0), (1, 1, 1), (1, 0, 0), (0, 1, 0), (1, 0, 1), (0, 1, 1), (0, 0, 1)]
        peers = [lax.rem(x + i, 2) * 4 + lax.rem(y + j, 2) * 2 + lax.rem(core + k, 2) for i, j, k in far]

    def kcopy(s):
        slot = lax.rem(s, SLOTS)
        return pltpu.make_async_copy(k_hbm.at[s], kbuf.at[slot], ksem.at[slot])

    def vcopy(s):
        slot = lax.rem(s, SLOTS)
        return pltpu.make_async_copy(v_hbm.at[s], vbuf.at[slot], vsem.at[slot])

    def vpieces():
        size = cache // PIECES
        slot = (rows - 1) % SLOTS
        return [
            pltpu.make_async_copy(v_hbm.at[rows - 1, :, pl.ds(i * size, size)], vbuf.at[slot, :, pl.ds(i * size, size)], last_sem.at[i])
            for i in range(PIECES)
        ]

    small = [
        pltpu.make_async_copy(src, dst, wsem.at[i])
        for i, (src, dst) in enumerate(
            [
                (x_hbm, x_ref),
                (ga_hbm, ga),
                (wq_hbm, wq),
                (table_hbm, table),
                (wo_hbm, wo),
                (gm_hbm, gm),
                (wg_hbm, wgu.at[:, :hidden]),
                (wu_hbm, wgu.at[:, hidden:]),
                (wd_hbm, wd),
            ]
        )
    ]
    for copy in small[:4]:
        copy.start()
    for s in range(SLOTS):
        kcopy(s).start()
        vcopy(s).start()
    for copy in small[4:]:
        copy.start()

    barrier = pltpu.get_barrier_semaphore()
    for peer in peers:
        pl.semaphore_signal(barrier, inc=1, device_id={"tp": peer}, device_id_type=MESH)

    for copy in small[:2]:
        copy.wait()
    xf[...] = x_ref[...].astype(F32)
    a = normed(xf[...], row_of(ga))
    for copy in small[2:4]:
        copy.wait()
    q = dot(a, wq[...]).astype(BF16).astype(F32)
    half = HEAD // 2
    lane = lax.broadcasted_iota(jnp.int32, q.shape, 1)
    other = jnp.where(lax.rem(lane, HEAD) < half, pltpu.roll(q, width - half, 1), pltpu.roll(q, half, 1))
    qf[...] = (q * table[0:1, :] + other * table[1:2, :]).astype(BF16).astype(F32)

    own = lax.broadcasted_iota(jnp.int32, (8, width), 1) // HEAD == lax.broadcasted_iota(jnp.int32, (8, width), 0)

    def score(s):
        query = jnp.where(own, jnp.broadcast_to(qf[pl.ds(s, 1), :], (8, width)), 0.0).astype(BF16)
        return dot(query, kbuf[lax.rem(s, SLOTS)])

    def weigh(wide):
        scaled = wide * HEAD**-0.5
        e = jnp.exp(scaled - jnp.max(scaled, -1, keepdims=True))
        return (e * (1.0 / jnp.sum(e, -1, keepdims=True))).astype(BF16)

    def keep(s, out):
        seen[pl.ds(s, 1), :] = jnp.sum(jnp.where(own, out, 0.0), 0, keepdims=True)

    def attend(s, wide):
        keep(s, dot_t(weigh(wide), vbuf[lax.rem(s, SLOTS)]))

    def send(kind, c, i, src, dst):
        return pltpu.make_async_remote_copy(
            src_ref=src,
            dst_ref=dst,
            send_sem=send_sem.at[slots[c][kind]],
            recv_sem=recv_sem.at[slots[c][kind]],
            device_id={"tp": peers[i]},
            device_id_type=MESH,
        )

    def others(kind, c, src, dst):
        return pltpu.make_async_remote_copy(
            src_ref=src.at[pl.ds(0, n - 1)],
            dst_ref=dst.at[pl.ds(0, n - 1)],
            send_sem=send_sem.at[slots[c][kind]],
            recv_sem=recv_sem.at[slots[c][kind]],
            device_id={"tp": peers[0]},
            device_id_type=MESH,
        )

    def arrive(kind, c, buf):
        others(kind, c, buf, buf).wait_recv()

    def total(buf):
        out = buf[0].astype(F32)
        for i in range(1, n):
            out = out + buf[i].astype(F32)
        return out

    def joined(buf):
        return jnp.concatenate([buf[i].astype(F32) for i in range(n)], 1)

    def spread(kind, c, buf):
        return [send(kind, c, i, buf.at[me], buf.at[me]) for i in range(n - 1)]

    def scatter(kind, c, src, dst):
        return [send(kind, c, i, src.at[peers[i]], dst.at[me]) for i in range(n - 1)]

    def start(copies):
        for copy in copies:
            copy.start()

    starts = [sum(chunk[0] for chunk in CHUNKS[:c]) for c in range(chunks)]
    parts = [slice(starts[c], starts[c] + CHUNKS[c][0]) for c in range(chunks)]
    tile = x_hbm.shape[1] // n
    mine = pl.ds(pl.multiple_of(me * tile, tile), tile)

    def send_term(half, c, term):
        if CHUNKS[c][1 + half]:
            staged, landed, _ = bufs[c][half]
            for i in range(n):
                staged[i] = term[:, i * tile : (i + 1) * tile].astype(BF16)
            start(scatter(2 * half, c, staged, landed))
            landed[me] = staged[me]
        else:
            (buf,) = bufs[c][half]
            buf[me] = term.astype(BF16)
            start(spread(2 * half, c, buf))

    def project(c):
        if c == 0:
            for copy in small[4:]:
                copy.wait()
            pl.semaphore_wait(barrier, n - 1)
        send_term(0, c, dot(seen[parts[c], :].astype(BF16), wo[...]))

    def reduce(half, c):
        _, landed, whole = bufs[c][half]
        arrive(2 * half, c, landed)
        if half == 0:
            before = xf[parts[c], mine]
        elif CHUNKS[c][1]:
            before = bufs[c][0][2][me].astype(F32)
        else:
            before = hf[parts[c], mine]
        whole[me] = (before + total(landed)).astype(BF16)
        start(spread(2 * half + 1, c, whole))

    def states(c):
        if CHUNKS[c][1]:
            arrive(1, c, bufs[c][0][2])
            return joined(bufs[c][0][2])
        (buf,) = bufs[c][0]
        arrive(0, c, buf)
        h = (xf[parts[c], :] + total(buf)).astype(BF16).astype(F32)
        hf[parts[c], :] = h
        return h

    def feed(*group):
        h = jnp.concatenate([states(c) for c in group], 0)
        b = normed(h, row_of(gm))
        both = dot(b, wgu[...])
        gate, up = both[:, :hidden], both[:, hidden:]
        product = (gate * (1.0 / (1.0 + jnp.exp(-gate))) * up).astype(BF16)
        term, at = dot(product, wd[...]), 0
        for c in group:
            send_term(1, c, term[at : at + CHUNKS[c][0], :])
            at += CHUNKS[c][0]

    def finish(c):
        if CHUNKS[c][2]:
            arrive(3, c, bufs[c][1][2])
            y_ref[parts[c], :] = joined(bufs[c][1][2]).astype(BF16)
        else:
            (buf,) = bufs[c][1]
            arrive(2, c, buf)
            y_ref[parts[c], :] = (hf[parts[c], :] + total(buf)).astype(BF16)

    stages = {"project": project, "reduce1": functools.partial(reduce, 0), "feed": feed, "reduce2": functools.partial(reduce, 1), "finish": finish}

    kcopy(0).wait()
    scores[0] = score(0)
    kcopy(SLOTS).start()

    def step(s, _):
        kcopy(s + 1).wait()
        vcopy(s).wait()
        wide = scores[lax.rem(s, 2)]
        scores[lax.rem(s + 1, 2)] = score(s + 1)
        attend(s, wide)

        @pl.when(s + 1 + SLOTS < rows)
        def _():
            kcopy(s + 1 + SLOTS).start()

        @pl.when(s + SLOTS < rows - 1)
        def _():
            vcopy(s + SLOTS).start()

        @pl.when(s + SLOTS == rows - 1)
        def _():
            start(vpieces())

        for row, names in EVENTS:
            if row < rows:

                @pl.when(s == row - 1)
                def _():
                    for name, *group in names:
                        stages[name](*group)

        return 0

    lax.fori_loop(0, rows - 1, step, 0)
    weights = weigh(scores[(rows - 1) % 2])
    size = cache // PIECES
    out = jnp.zeros((8, width), F32)
    for i, copy in enumerate(vpieces()):
        copy.wait()
        out = out + dot_t(weights[:, i * size : (i + 1) * size], vbuf[(rows - 1) % SLOTS, :, i * size : (i + 1) * size])
    keep(rows - 1, out)
    for row, names in EVENTS:
        if row == rows:
            for name, *group in names:
                if name == "project":
                    pl.when(me >= 0)(functools.partial(project, *group))
                else:
                    stages[name](*group)

    for c in range(chunks):
        for half in range(2):
            own_buf, *more = bufs[c][half]
            others(2 * half, c, own_buf, own_buf).wait_send()
            if more:
                others(2 * half + 1, c, more[1], more[1]).wait_send()


def solution(mesh):
    n = mesh.shape["tp"]

    def step(x, k_cache, v_cache, gain_a, wq, wo, gain_m, w_gate, w_up, w_down):
        rows, cache, heads, head = k_cache.shape
        d, width, hidden = x.shape[1], heads * head, w_gate.shape[1]
        flat = lambda t: t.transpose(0, 2, 3, 1).reshape(rows, width, cache)
        table = jnp.asarray(turn_table(cache - 1, heads))
        exchanges = sum(2 if split else 1 for _, *splits in CHUNKS for split in splits)
        scratch = [
            pltpu.VMEM((SLOTS, width, cache), BF16),
            pltpu.VMEM((SLOTS, width, cache), BF16),
            pltpu.VMEM((rows, d), BF16),
            pltpu.VMEM((d // 128, 128), BF16),
            pltpu.VMEM((d // 128, 128), BF16),
            pltpu.VMEM((2, width), F32),
            pltpu.VMEM((d, width), BF16),
            pltpu.VMEM((width, d), BF16),
            pltpu.VMEM((d, 2 * hidden), BF16),
            pltpu.VMEM((hidden, d), BF16),
            pltpu.VMEM((rows, d), F32),
            pltpu.VMEM((rows, d), F32),
            pltpu.VMEM((rows, width), F32),
            pltpu.VMEM((rows, width), F32),
            pltpu.VMEM((2, 8, cache), F32),
            pltpu.SemaphoreType.DMA((SLOTS,)),
            pltpu.SemaphoreType.DMA((SLOTS,)),
            pltpu.SemaphoreType.DMA((9,)),
            pltpu.SemaphoreType.DMA((exchanges,)),
            pltpu.SemaphoreType.DMA((exchanges,)),
            pltpu.SemaphoreType.DMA((PIECES,)),
        ]
        for size, *splits in CHUNKS:
            for split in splits:
                scratch += [pltpu.VMEM((n, size, d // n), BF16)] * 3 if split else [pltpu.VMEM((n, size, d), BF16)]
        return pl.pallas_call(
            functools.partial(kernel, n),
            out_shape=pltpu.VMEM((rows, d), BF16),
            in_specs=[pl.BlockSpec(memory_space=pl.ANY)] * 11,
            out_specs=pl.BlockSpec(memory_space=pltpu.VMEM),
            scratch_shapes=scratch,
            compiler_params=pltpu.CompilerParams(collective_id=0, has_side_effects=True, vmem_limit_bytes=58_000_000),
        )(flat(k_cache), flat(v_cache), x, gain_a.reshape(d // 128, 128), wq, wo, gain_m.reshape(d // 128, 128), w_gate, w_up, w_down, table)

    states, cache, columns, rows_of = P("dp", None), P("dp", None, "tp", None), P(None, "tp"), P("tp", None)
    return jax.shard_map(
        step,
        mesh=mesh,
        in_specs=(states, cache, cache, P(None), columns, rows_of, P(None), columns, columns, rows_of),
        out_specs=states,
        check_vma=False,
    )
```
